32 devices in a mesh: wide: 8 (over z, y), narrow: 4 (over x, core).
Axes of the slice: x: 2, y: 2, z: 4, core: 2. Of those that a mesh axis runs over, the one named last changes fastest.
Arguments:
- tokens: bfloat16 [4096, 2048], P(('wide', 'narrow')), may hold values from -6 to 6
- expert_ids: int32 [4096, 10], P(('wide', 'narrow')), may hold values from 0 to 255, all different within a row; in each aligned block of 128 rows (0 to 127, 128 to 255, ...) at most 7 rows name the same one
- combine: int32 [4096, 10], P(('wide', 'narrow')), may hold values from 8 to 63
- w_gate: bfloat16 [256, 2048, 512], P(('wide', 'narrow')), may hold values from -0.125 to 0.125
- w_up: bfloat16 [256, 2048, 512], P(('wide', 'narrow')), may hold values from -0.125 to 0.125
- w_down: bfloat16 [256, 512, 2048], P(('wide', 'narrow')), may hold values from -0.25 to 0.25
- shared_gate_up: bfloat16 [2, 2048, 512], P(None, None, 'narrow'), may hold values from -0.125 to 0.125
- shared_down: bfloat16 [512, 2048], P('narrow'), may hold values from -0.25 to 0.25
- gate_vector: bfloat16 [2048], replicated, may hold values from -0.25 to 0.25
Outputs:
- layer_out: bfloat16 [4096, 2048], P(('wide', 'narrow'))
The draws below stay inside these ranges and needn't reach their ends.
Inputs may be any that keep to these rules, and one draw needn't show every extreme that they name: `expert_ids`: each row names 10 different experts. Among the 128 rows of one device no expert is named more than 7 times, and in every draw some device names some expert exactly 7 times. `combine`: an assignment's weight is its value divided by 256.
All inputs are finite; a program needn't handle non-finite values.
Results may differ from the reference program's by a relative error of at most 0.0054.
Values may be sent and summed in bfloat16 or wider, within the bound.
No kernel may reach another device: no remote copies, remote signals or barrier semaphores. Data moves between devices by JAX's collectives and lax.ppermute only.
A program may use at most 128 MiB of HBM per device.

```python
import math
import jax
import jax.numpy as jnp
import numpy as np
from jax import lax

D = 2048
FF = 512
SH = 512
TOP = 10
EXPERTS = 256
TOK_DEV = 128
CAP = 7
TOKENS = 4096
DEVICES = 32


def touch_ends(result, rng, smallest, high):
    longest = result.shape.index(max(result.shape))
    spots = []
    for shift in (0, 1):
        where = [jax.random.randint(jax.random.fold_in(rng, axis), (), 0, length) for axis, length in enumerate(result.shape)]
        where[longest] = (where[longest] + shift) % result.shape[longest]
        spots.append(tuple(where))
    return result.at[spots[0]].set(smallest).at[spots[1]].set(high)


def block_scale(rng, shape, shards, least, top_value):
    def one(dim, shards_of):
        heights = jax.random.uniform(jax.random.fold_in(jax.random.fold_in(rng, 6), dim), (shards_of,), jnp.float32, least / len(shards), top_value / len(shards))
        return jnp.repeat(jnp.exp(heights), shape[dim] // shards_of).reshape((-1,) + (1,) * (len(shape) - dim - 1))

    factor_of = one(*shards[0])
    for cut in shards[1:]:
        factor_of = factor_of * one(*cut)
    return factor_of


def deal_out(key, own, number, rows, amount, top, bound, lean):
    sequence = jax.random.permutation(key, amount)
    packed, ordinary = portions_of(amount, rows * top, bound, lean, True), portions_of(amount, rows * top, bound, lean, False)
    places = jnp.arange(amount)

    def named(tallies, offset_by):
        used = int((tallies > 0).sum())
        fixed = max(1, used // 4)
        moved = fixed + (places - fixed + offset_by * (used - fixed)) % max(1, amount - fixed)
        return jnp.zeros((amount,), jnp.int32).at[sequence[jnp.where(places < fixed, places, moved)]].set(jnp.asarray(tallies, jnp.int32))

    tallies = jnp.where(number % 4 == 0, named(packed, number // 4), named(ordinary, number - number // 4 - 1))
    mixed = jax.random.permutation(jax.random.fold_in(own, 3), amount)
    source_of, taker = mixed[0:amount // 2 * 2:2], mixed[1:amount // 2 * 2:2]
    margin = jnp.minimum(tallies[source_of] - 1, bound - tallies[taker]) // 2
    margin = jnp.where((source_of == sequence[0]) | (taker == sequence[0]) | (tallies[taker] == 0), 0, jnp.maximum(margin, 0))
    moved = jax.random.randint(jax.random.fold_in(own, 4), (amount // 2,), 0, 1 << 20) % (margin + 1)
    tallies = tallies.at[source_of].add(-moved).at[taker].add(moved)
    items = jnp.searchsorted(jnp.cumsum(tallies), jnp.arange(rows * top), side="right").astype(jnp.int32)
    listing = items.reshape(top, rows).T
    listing = listing[jax.random.permutation(jax.random.fold_in(own, 1), rows)]
    offset_by = jax.random.randint(jax.random.fold_in(own, 2), (rows, 1), 0, top)
    return jnp.take_along_axis(listing, (jnp.arange(top)[None, :] + offset_by) % top, axis=1)


def portions_of(count, total, most, skew, full):
    loads = [(1 << 20) // math.isqrt(rank ** skew) + 1 for rank in range(1, count + 1)]
    largest = most if full else min(most, max(-(-total // count), total * loads[0] // sum(loads)))
    least = 1 if total - largest >= count - 1 else 0
    given, spare = [largest] + [least] * (count - 1), total - largest - least * (count - 1)
    while spare > 0:
        movable = [i for i in range(1, count) if given[i] < largest] or [i for i in range(1, count) if given[i] < most]
        mass, left = sum([loads[i] for i in movable]), spare
        for i in movable:
            extra = min(most - given[i], max(1, left * loads[i] // mass), spare)
            given[i] = given[i] + extra
            spare = spare - extra
    return np.array(given)


def noise(own_key, dims, scale, limit, split=(), held_as=jnp.bfloat16):
    values = jax.random.normal(own_key, dims, jnp.float32) * scale
    if len(split) > 0:
        values = block_scale(own_key, dims, split, -0.22, 0.18) * values
    return jnp.clip(values, min=-limit, max=limit).astype(held_as)


def setup_inputs(seed: int = 0) -> dict:
    key_of = jax.random.split(jax.random.key(seed), 10)
    tokens = noise(key_of[0], (TOKENS, D), 1.0, 6.0, ((0, 32),))
    expert_ids_keys = jax.random.split(jax.random.fold_in(key_of[1], 1), TOKENS // TOK_DEV)
    expert_ids_turns = jax.random.permutation(jax.random.fold_in(key_of[1], 3), TOKENS // TOK_DEV)
    expert_ids = jax.vmap(lambda own, number: deal_out(jax.random.fold_in(key_of[1], 2), own, number, TOK_DEV, EXPERTS, TOP, CAP, 2))(expert_ids_keys, expert_ids_turns).reshape((TOKENS, TOP))
    combine = touch_ends(jax.random.randint(key_of[2], (TOKENS, TOP), 8, 64), jax.random.fold_in(key_of[2], 1), 8, 63).astype(jnp.int32)
    w_gate = noise(key_of[3], (EXPERTS, D, FF), D ** -0.5, 0.125, ((0, 32),))
    w_up = noise(key_of[4], (EXPERTS, D, FF), D ** -0.5, 0.125, ((0, 32),))
    w_down = noise(key_of[5], (EXPERTS, FF, D), FF ** -0.5, 0.25, ((0, 32),))
    shared_gate_up = noise(key_of[6], (2, D, SH), D ** -0.5, 0.125, ((2, 4),))
    shared_down = noise(key_of[7], (SH, D), SH ** -0.5, 0.25, ((0, 4),))
    gate_vector = noise(key_of[8], (D,), (D // 4) ** -0.5, 0.25)
    return {"tokens": tokens, "expert_ids": expert_ids, "combine": combine, "w_gate": w_gate, "w_up": w_up, "w_down": w_down, "shared_gate_up": shared_gate_up, "shared_down": shared_down, "gate_vector": gate_vector}


def slot_order(flat_ids, experts_total):
    columns = jnp.arange(experts_total, dtype=jnp.int32)
    onehot = (flat_ids[:, None] == columns[None, :]).astype(jnp.int32)
    before = jnp.cumsum(onehot, axis=0) - onehot
    return jnp.sum(before * onehot, axis=1).astype(jnp.int32)


def place_block(block):
    return slot_order(block, EXPERTS)


def reference(tokens, expert_ids, combine, w_gate, w_up, w_down, shared_gate_up, shared_down, gate_vector):
    blocks = expert_ids.reshape(DEVICES, TOK_DEV * TOP).astype(jnp.int32)
    positions = lax.map(place_block, blocks)
    device_of = jnp.arange(DEVICES, dtype=jnp.int32)[:, None]
    slot_index = ((blocks * DEVICES + device_of) * CAP + positions).reshape(-1).astype(jnp.int32)
    within = jnp.arange(TOK_DEV * TOP, dtype=jnp.int32)[None, :] // TOP
    owners = (device_of * TOK_DEV + within).reshape(-1).astype(jnp.int32)
    slot_total = EXPERTS * DEVICES * CAP
    slot_token = jnp.full((slot_total,), -1, jnp.int32).at[slot_index].set(owners)
    slot_weight = jnp.zeros((slot_total,), jnp.float32).at[slot_index].set(
        combine.reshape(-1).astype(jnp.float32) / 256.0)
    span = DEVICES * CAP

    def expert_step(running, inputs):
        gate_w, up_w, down_w, expert = inputs
        token_rows = lax.dynamic_slice_in_dim(slot_token, (expert * span).astype(jnp.int32), span, 0)
        row_weights = lax.dynamic_slice_in_dim(slot_weight, (expert * span).astype(jnp.int32), span, 0)
        safe_rows = jnp.maximum(token_rows, 0)
        chosen = tokens[safe_rows]
        gate_part = jnp.dot(chosen, gate_w, preferred_element_type=jnp.float32)
        up_part = jnp.dot(chosen, up_w, preferred_element_type=jnp.float32)
        hidden = (jax.nn.silu(gate_part) * up_part).astype(jnp.bfloat16)
        produced = jnp.dot(hidden, down_w, preferred_element_type=jnp.float32).astype(jnp.bfloat16)
        running = running.at[safe_rows].add(row_weights[:, None] * produced.astype(jnp.float32))
        return running, None

    routed, unused = lax.scan(expert_step, jnp.zeros((TOKENS, D), jnp.float32),
                              (w_gate, w_up, w_down, jnp.arange(EXPERTS, dtype=jnp.int32)))
    shared_gate = jnp.dot(tokens, shared_gate_up[0], preferred_element_type=jnp.float32)
    shared_up = jnp.dot(tokens, shared_gate_up[1], preferred_element_type=jnp.float32)
    shared_hidden = (jax.nn.silu(shared_gate) * shared_up).astype(jnp.bfloat16)
    shared_out = jnp.dot(shared_hidden, shared_down, preferred_element_type=jnp.float32)
    shared_scale = jax.nn.sigmoid(jnp.dot(tokens, gate_vector, preferred_element_type=jnp.float32))
    return (routed + shared_scale[:, None] * shared_out).astype(jnp.bfloat16)
```

```python
import functools
import jax
import jax.numpy as jnp
from jax import lax
from jax.experimental import pallas as pl
from jax.experimental.pallas import tpu as pltpu
from jax.sharding import PartitionSpec as P


CAP = 7
AXES = ("wide", "narrow")
BF = jnp.bfloat16
F32 = jnp.float32
META = 8
SLOTS = 8


def slot_order(flat_ids, experts_total):
    columns = jnp.arange(experts_total, dtype=jnp.int32)
    onehot = (flat_ids[:, None] == columns[None, :]).astype(jnp.int32)
    before = jnp.cumsum(onehot, axis=0) - onehot
    return jnp.sum(before * onehot, axis=1)


def expert_block(received, w_gate, w_up, w_down):
    gate_part = jnp.einsum("secd,edf->secf", received, w_gate, preferred_element_type=F32)
    up_part = jnp.einsum("secd,edf->secf", received, w_up, preferred_element_type=F32)
    hidden = (jax.nn.silu(gate_part) * up_part).astype(BF)
    return jnp.einsum("secf,efd->secd", hidden, w_down, preferred_element_type=F32).astype(BF)


def by_all_to_all(
    tokens, expert_ids, combine, w_gate, w_up, w_down, shared_gate_up, shared_down, gate_vector
):
    tok_rows, model_width = tokens.shape
    top_count = expert_ids.shape[1]
    devices = lax.axis_size(AXES)
    local_experts = w_gate.shape[0]
    experts_total = local_experts * devices
    flat_ids = expert_ids.reshape(-1)
    positions = slot_order(flat_ids, experts_total)
    slot_index = flat_ids * CAP + positions
    repeated = jnp.repeat(tokens, top_count, axis=0)
    outgoing = jnp.zeros((experts_total * CAP, model_width), BF).at[slot_index].set(repeated)
    outgoing = outgoing.reshape(devices, local_experts, CAP, model_width)
    produced = expert_block(
        lax.all_to_all(outgoing, AXES, split_axis=0, concat_axis=0, tiled=True),
        w_gate,
        w_up,
        w_down,
    )
    returned = lax.all_to_all(produced, AXES, split_axis=0, concat_axis=0, tiled=True)
    returned = returned.reshape(experts_total * CAP, model_width)
    returned_rows = returned[slot_index].reshape(tok_rows, top_count, model_width)
    mix_weights = combine.astype(F32) / 256.0
    routed = jnp.sum(returned_rows.astype(F32) * mix_weights[:, :, None], axis=1)
    shared_scale = jax.nn.sigmoid(jnp.dot(tokens, gate_vector, preferred_element_type=F32))
    gate_up = jnp.einsum(
        "td,gdn->gtn",
        tokens,
        lax.all_gather(shared_gate_up, "narrow", axis=2, tiled=True),
        preferred_element_type=F32,
    )
    shared_hidden = (jax.nn.silu(gate_up[0]) * gate_up[1]).astype(BF)
    shared_out = jnp.dot(
        shared_hidden,
        lax.all_gather(shared_down, "narrow", axis=0, tiled=True),
        preferred_element_type=F32,
    )
    layer_out = routed + shared_scale[:, None] * shared_out
    return layer_out.astype(BF)


def dot(a, b, dims=(((1,), (0,)), ((), ()))):
    return lax.dot_general(a, b, dims, preferred_element_type=F32)


def select_kernel(first_ref, own_ref, sib_ref, x_ref, cw_ref, *, rows, top, experts):
    first = first_ref[0].astype(F32)
    r = lax.broadcasted_iota(jnp.int32, (rows, rows), 0)
    c = lax.broadcasted_iota(jnp.int32, (rows, rows), 1)
    upper = jnp.where(r < c, 1.0, 0.0).astype(BF)
    mine = lax.broadcasted_iota(jnp.int32, (experts, 1, rows), 0).astype(F32) + first
    slot = lax.broadcasted_iota(jnp.int32, (experts, SLOTS, rows), 1).astype(F32)
    zero = jnp.zeros((experts, SLOTS, rows), F32)
    blocks = [own_ref.at[i] for i in range(4)] + [sib_ref.at[i] for i in range(4)]

    def table(meta, at):
        parts = []
        for k0 in range(0, top, META):
            n = min(META, top - k0)
            lanes = (at + k0 // META) * rows
            parts.append(meta[0:n, lanes : lanes + rows])
        return jnp.concatenate(parts, axis=0)

    per = -(-top // META)
    for pair in range(4):
        halves, weighted = [], []
        for b in range(2):
            ref = blocks[2 * pair + b]
            meta = ref[rows : rows + META, 0 : 2 * per * rows].astype(F32)
            ids, mix = table(meta, 0), table(meta, per)
            match = jnp.where(ids[None] == mine, 1.0, 0.0)
            hit = jnp.sum(match, axis=1)
            mix_of = jnp.sum(match * mix[None], axis=1) * (1.0 / 256.0)
            before = dot(hit.astype(BF), upper)
            here = jnp.where((before[:, None, :] == slot) & (hit[:, None, :] > 0.0), 1.0, 0.0)
            halves.append(here)
            weighted.append(here * mix_of[:, None, :])
        sel = jnp.concatenate(
            [
                jnp.concatenate([halves[0], zero], axis=2),
                jnp.concatenate([zero, halves[1]], axis=2),
            ],
            axis=1,
        )
        cw = jnp.concatenate(
            [
                jnp.concatenate([weighted[0], zero], axis=2),
                jnp.concatenate([zero, weighted[1]], axis=2),
            ],
            axis=1,
        )
        sel = sel.reshape(experts * 2 * SLOTS, 2 * rows).astype(BF)
        cw_ref[pair] = cw.reshape(experts * 2 * SLOTS, 2 * rows).astype(BF)
        toks = jnp.concatenate([blocks[2 * pair][0:rows, :], blocks[2 * pair + 1][0:rows, :]], axis=0)
        picked = dot(sel, toks).astype(BF)
        x_ref[:, 2 * SLOTS * pair : 2 * SLOTS * (pair + 1), :] = picked.reshape(
            experts, 2 * SLOTS, picked.shape[1]
        )


def select(first, own, sib, rows, top, experts):
    width = own.shape[2]
    vm = pl.BlockSpec(memory_space=pltpu.VMEM)
    return pl.pallas_call(
        functools.partial(select_kernel, rows=rows, top=top, experts=experts),
        out_shape=(
            jax.ShapeDtypeStruct((experts, 8 * SLOTS, width), BF),
            jax.ShapeDtypeStruct((4, experts * 2 * SLOTS, 2 * rows), BF),
        ),
        in_specs=[pl.BlockSpec(memory_space=pltpu.SMEM), vm, vm],
        out_specs=(vm, vm),
        cost_estimate=pl.CostEstimate(
            flops=2 * 8 * rows * 2 * experts * SLOTS * width,
            bytes_accessed=10 * own.size,
            transcendentals=0,
        ),
        name="select",
    )(first, own, sib)


def expert_kernel(*refs, columns):
    xs, (wg, wu, wd), ys = refs[:columns], refs[columns : columns + 3], refs[columns + 3 :]
    x = jnp.concatenate([ref[0] for ref in xs], axis=0)
    gate = dot(x, wg[0])
    up = dot(x, wu[0])
    hidden = (gate / (1.0 + jnp.exp(-gate)) * up).astype(BF)
    out = dot(hidden, wd[0]).astype(BF)
    n = xs[0].shape[1]
    for j in range(columns):
        ys[j][0] = out[j * n : (j + 1) * n]


def run_experts(xs, w_gate, w_up, w_down):
    columns = len(xs)
    experts, n, width = xs[0].shape
    hidden = w_gate.shape[2]
    blk = pl.BlockSpec((1, n, width), lambda e: (e, 0, 0))
    return pl.pallas_call(
        functools.partial(expert_kernel, columns=columns),
        grid=(experts,),
        out_shape=[jax.ShapeDtypeStruct(xs[0].shape, BF)] * columns,
        in_specs=[blk] * columns
        + [
            pl.BlockSpec((1, width, hidden), lambda e: (e, 0, 0)),
            pl.BlockSpec((1, width, hidden), lambda e: (e, 0, 0)),
            pl.BlockSpec((1, hidden, width), lambda e: (e, 0, 0)),
        ],
        out_specs=[blk] * columns,
        cost_estimate=pl.CostEstimate(
            flops=6 * experts * columns * n * width * hidden,
            bytes_accessed=2 * (3 * w_gate.size + 2 * columns * xs[0].size),
            transcendentals=experts * columns * n * hidden,
        ),
        name="experts",
    )(*xs, w_gate, w_up, w_down)


def shared_kernel(toks_a, toks_b, wgu_ref, wd_ref, gv_ref, out_ref, *, rows):
    for b in range(4):
        src = (toks_a, toks_b)[b // 2]
        x = src[b % 2][0:rows, :]
        gate = dot(x, wgu_ref[0])
        up = dot(x, wgu_ref[1])
        hidden = (gate / (1.0 + jnp.exp(-gate)) * up).astype(BF)
        scale = 1.0 / (1.0 + jnp.exp(-dot(x, gv_ref[...])[:, 0:1]))
        out_ref[b] = scale * dot(hidden, wd_ref[...])


def run_shared(own, sib, shared_gate_up, shared_down, gate_columns, rows):
    width = own.shape[2]
    return pl.pallas_call(
        functools.partial(shared_kernel, rows=rows),
        grid=(1,),
        out_shape=jax.ShapeDtypeStruct((4, rows, width), F32),
        in_specs=[
            pl.BlockSpec((2,) + own.shape[1:], lambda i: (0, 0, 0)),
            pl.BlockSpec((2,) + own.shape[1:], lambda i: (0, 0, 0)),
            pl.BlockSpec(shared_gate_up.shape, lambda i: (0, 0, 0)),
            pl.BlockSpec(shared_down.shape, lambda i: (0, 0)),
            pl.BlockSpec(gate_columns.shape, lambda i: (0, 0)),
        ],
        out_specs=pl.BlockSpec((4, rows, width), lambda i: (0, 0, 0)),
        cost_estimate=pl.CostEstimate(
            flops=2 * 4 * rows * width * 512, bytes_accessed=8 * 2**20, transcendentals=0
        ),
        name="shared",
    )(own, sib, shared_gate_up, shared_down, gate_columns)


def mix_kernel(*refs, rows, with_shared):
    if with_shared:
        y_ref, cw_ref, sh_ref, own_ref, sib_ref = refs
    else:
        y_ref, cw_ref, own_ref, sib_ref = refs
    for pair in range(4):
        y = y_ref[:, 2 * SLOTS * pair : 2 * SLOTS * (pair + 1), :]
        y = y.reshape(y.shape[0] * y.shape[1], y.shape[2])
        part = dot(cw_ref[pair], y, (((0,), (0,)), ((), ())))
        dst = own_ref if pair < 2 else sib_ref
        for b in range(2):
            piece = part[b * rows : (b + 1) * rows]
            if with_shared and pair % 2 == 0:
                piece = piece + sh_ref[pair + b]
            dst[2 * (pair % 2) + b] = piece.astype(BF)


def mix(y, cw, rows, shared=None):
    width = y.shape[2]
    vm = pl.BlockSpec(memory_space=pltpu.VMEM)
    ins = (y, cw) if shared is None else (y, cw, shared)
    return pl.pallas_call(
        functools.partial(mix_kernel, rows=rows, with_shared=shared is not None),
        out_shape=[jax.ShapeDtypeStruct((4, rows, width), BF)] * 2,
        in_specs=[vm] * len(ins),
        out_specs=[vm, vm],
        cost_estimate=pl.CostEstimate(
            flops=2 * 8 * rows * 2 * y.shape[0] * SLOTS * width,
            bytes_accessed=6 * y.size,
            transcendentals=0,
        ),
        name="mix",
    )(*ins)


class Grid:
    def __init__(self, mesh):
        flat = list(mesh.devices.flat)
        self.at = [tuple(d.coords) + (d.core_on_chip,) for d in flat]
        low = [min(p[i] for p in self.at) for i in range(4)]
        self.at = [tuple(p[i] - low[i] for i in range(4)) for p in self.at]
        self.index = {p: i for i, p in enumerate(self.at)}
        self.size = tuple(max(p[i] for p in self.at) + 1 for i in range(4))

    def perm(self, axis, shift):
        pairs = []
        for i, p in enumerate(self.at):
            q = list(p)
            q[axis] = (q[axis] + shift) % self.size[axis]
            pairs.append((i, self.index[tuple(q)]))
        return pairs


def by_neighbours(
    grid,
    tokens,
    expert_ids,
    combine,
    w_gate,
    w_up,
    w_down,
    shared_gate_up,
    shared_down,
    gate_vector,
):
    rows, width = tokens.shape
    top = expert_ids.shape[1]
    experts = w_gate.shape[0]
    depth = grid.size[2]
    half = rows // 2

    def send(value, axis, shift=1):
        return lax.ppermute(value, AXES, grid.perm(axis, shift))

    first = (lax.axis_index(AXES) * experts).astype(jnp.int32).reshape(1)
    per = -(-top // META)

    def tile(values):
        t = jnp.pad(values.T.astype(BF), ((0, per * META - top), (0, 0)))
        return t.reshape(per, META, rows).transpose(1, 0, 2).reshape(META, per * rows)

    meta = jnp.concatenate([tile(expert_ids), tile(combine)], axis=1)
    meta = jnp.pad(meta, ((0, 0), (0, width - meta.shape[1])))
    own = jnp.concatenate([tokens, meta], axis=0)

    order = column_order(depth)
    cols, picked, weights = {0: own}, {}, {}
    shared = None
    for k in order[1:]:
        cols[k] = send(own, 2, k)
    for j in order:
        o = cols[j]
        x, y = send(o, 0), send(o, 1)
        d0, d1 = send(x[:half], 1), send(y[half:], 0)
        mine = jnp.stack([o, x, y, jnp.concatenate([d0, d1], axis=0)])
        theirs = send(mine, 3)
        picked[j], weights[j] = select(first, mine, theirs, rows, top, experts)
        if j == 0:
            gate_columns = jnp.broadcast_to(gate_vector[:, None], (width, 128))
            shared = run_shared(mine, theirs, shared_gate_up, shared_down, gate_columns, rows)

    outs = run_experts([picked[j] for j in range(depth)], w_gate, w_up, w_down)

    total = None
    for j in order[::-1]:
        r, q = mix(outs[j], weights[j], rows, shared if j == 0 else None)
        got = send(q, 3)
        add = lambda i: r[i].astype(F32) + got[i].astype(F32)
        d = add(3).astype(BF)
        d0, d1 = send(d[:half], 1), send(d[half:], 0)
        x, y = add(1), add(2)
        x = jnp.concatenate([x[:half] + d0.astype(F32), x[half:]], axis=0).astype(BF)
        y = jnp.concatenate([y[:half], y[half:] + d1.astype(F32)], axis=0).astype(BF)
        o = add(0) + send(x, 0).astype(F32) + send(y, 1).astype(F32)
        if j:
            o = send(o.astype(BF), 2, -j).astype(F32)
        total = o if total is None else total + o
    return total.astype(BF)


def column_order(depth):
    near = sorted({1 % depth, depth - 1} - {0})
    return [0] + near + [k for k in range(1, depth) if k not in near]


def solution(mesh):
    grid = Grid(mesh)
    planar = grid.size[0] == 2 and grid.size[1] == 2 and grid.size[3] == 2

    def body(*args):
        return by_neighbours(grid, *args) if planar else by_all_to_all(*args)

    return jax.shard_map(
        body,
        mesh=mesh,
        in_specs=(
            P(AXES, None),
            P(AXES, None),
            P(AXES, None),
            P(AXES, None, None),
            P(AXES, None, None),
            P(AXES, None, None),
            P(None, None, "narrow"),
            P("narrow", None),
            P(),
        ),
        out_specs=P(AXES, None),
        check_vma=False,
    )
```

```python
import functools
import jax
import jax.numpy as jnp
from jax import lax
from jax.experimental import pallas as pl
from jax.experimental.pallas import tpu as pltpu
from jax.sharding import PartitionSpec as P


CAP = 7
AXES = ("wide", "narrow")
BF = jnp.bfloat16
F32 = jnp.float32
META = 8
SLOTS = 8


def slot_order(flat_ids, experts_total):
    columns = jnp.arange(experts_total, dtype=jnp.int32)
    onehot = (flat_ids[:, None] == columns[None, :]).astype(jnp.int32)
    before = jnp.cumsum(onehot, axis=0) - onehot
    return jnp.sum(before * onehot, axis=1)


def expert_block(received, w_gate, w_up, w_down):
    gate_part = jnp.einsum("secd,edf->secf", received, w_gate, preferred_element_type=F32)
    up_part = jnp.einsum("secd,edf->secf", received, w_up, preferred_element_type=F32)
    hidden = (jax.nn.silu(gate_part) * up_part).astype(BF)
    return jnp.einsum("secf,efd->secd", hidden, w_down, preferred_element_type=F32).astype(BF)


def by_all_to_all(
    tokens, expert_ids, combine, w_gate, w_up, w_down, shared_gate_up, shared_down, gate_vector
):
    tok_rows, model_width = tokens.shape
    top_count = expert_ids.shape[1]
    devices = lax.axis_size(AXES)
    local_experts = w_gate.shape[0]
    experts_total = local_experts * devices
    flat_ids = expert_ids.reshape(-1)
    positions = slot_order(flat_ids, experts_total)
    slot_index = flat_ids * CAP + positions
    repeated = jnp.repeat(tokens, top_count, axis=0)
    outgoing = jnp.zeros((experts_total * CAP, model_width), BF).at[slot_index].set(repeated)
    outgoing = outgoing.reshape(devices, local_experts, CAP, model_width)
    produced = expert_block(
        lax.all_to_all(outgoing, AXES, split_axis=0, concat_axis=0, tiled=True),
        w_gate,
        w_up,
        w_down,
    )
    returned = lax.all_to_all(produced, AXES, split_axis=0, concat_axis=0, tiled=True)
    returned = returned.reshape(experts_total * CAP, model_width)
    returned_rows = returned[slot_index].reshape(tok_rows, top_count, model_width)
    mix_weights = combine.astype(F32) / 256.0
    routed = jnp.sum(returned_rows.astype(F32) * mix_weights[:, :, None], axis=1)
    shared_scale = jax.nn.sigmoid(jnp.dot(tokens, gate_vector, preferred_element_type=F32))
    gate_up = jnp.einsum(
        "td,gdn->gtn",
        tokens,
        lax.all_gather(shared_gate_up, "narrow", axis=2, tiled=True),
        preferred_element_type=F32,
    )
    shared_hidden = (jax.nn.silu(gate_up[0]) * gate_up[1]).astype(BF)
    shared_out = jnp.dot(
        shared_hidden,
        lax.all_gather(shared_down, "narrow", axis=0, tiled=True),
        preferred_element_type=F32,
    )
    layer_out = routed + shared_scale[:, None] * shared_out
    return layer_out.astype(BF)


def dot(a, b, dims=(((1,), (0,)), ((), ()))):
    return lax.dot_general(a, b, dims, preferred_element_type=F32)


def split_block(refs, rows):
    if len(refs) == 1:
        return refs[0][0:rows, :], refs[0][rows : rows + META, :]
    top, rest = refs
    cut = rows - top.shape[0]
    return jnp.concatenate([top[...], rest[0:cut, :]], axis=0), rest[cut : cut + META, :]


def select_kernel(me_ref, *refs, counts, flip, rows, top, experts):
    blocks, at = [], 0
    for n in counts:
        blocks.append(split_block(refs[at : at + n], rows))
        at += n
    own_ref, sib_ref, cw_ref = refs[at:]
    r = lax.broadcasted_iota(jnp.int32, (rows, rows), 0)
    c = lax.broadcasted_iota(jnp.int32, (rows, rows), 1)
    upper = jnp.where(r < c, 1.0, 0.0).astype(BF)
    e = lax.broadcasted_iota(jnp.int32, (2 * experts, 1, rows), 0)
    me = me_ref[0]
    sib = jnp.bitwise_xor(me, flip)
    mine = jnp.where(e < experts, e + me * experts, e - experts + sib * experts).astype(F32)
    slot = lax.broadcasted_iota(jnp.int32, (2 * experts, SLOTS, rows), 1).astype(F32)
    zero = jnp.zeros((2 * experts, SLOTS, rows), F32)
    per = -(-top // META)

    def table(meta, at):
        parts = []
        for k0 in range(0, top, META):
            n = min(META, top - k0)
            lanes = (at + k0 // META) * rows
            parts.append(meta[0:n, lanes : lanes + rows])
        return jnp.concatenate(parts, axis=0)

    def spread(pieces):
        wide = [jnp.concatenate([pieces[0], zero], 2), jnp.concatenate([zero, pieces[1]], 2)]
        both = jnp.concatenate(wide, axis=1)
        return both.reshape(4 * experts * SLOTS, 2 * rows).astype(BF)

    for pair in range(2):
        halves, weighted = [], []
        for toks, meta in blocks[2 * pair : 2 * pair + 2]:
            meta = meta[:, 0 : 2 * per * rows].astype(F32)
            ids, part = table(meta, 0), table(meta, per)
            match = jnp.where(ids[None] == mine, 1.0, 0.0)
            hit = jnp.sum(match, axis=1)
            part_of = jnp.sum(match * part[None], axis=1) * (1.0 / 256.0)
            before = dot(hit.astype(BF), upper)
            here = jnp.where((before[:, None, :] == slot) & (hit[:, None, :] > 0.0), 1.0, 0.0)
            halves.append(here)
            weighted.append(here * part_of[:, None, :])
        cw_ref[pair] = spread(weighted)
        toks = jnp.concatenate([blocks[2 * pair][0], blocks[2 * pair + 1][0]], axis=0)
        picked = dot(spread(halves), toks).astype(BF)
        picked = picked.reshape(2 * experts, 2 * SLOTS, picked.shape[1])
        own_ref[:, 2 * SLOTS * pair : 2 * SLOTS * (pair + 1), :] = picked[:experts]
        sib_ref[:, 2 * SLOTS * pair : 2 * SLOTS * (pair + 1), :] = picked[experts:]


def select(me, blocks, flip, rows, top, experts):
    width = blocks[0][0].shape[1]
    vm = pl.BlockSpec(memory_space=pltpu.VMEM)
    flat = [piece for block in blocks for piece in block]
    return pl.pallas_call(
        functools.partial(
            select_kernel,
            counts=[len(b) for b in blocks],
            flip=flip,
            rows=rows,
            top=top,
            experts=experts,
        ),
        out_shape=(
            jax.ShapeDtypeStruct((experts, 4 * SLOTS, width), BF),
            jax.ShapeDtypeStruct((experts, 4 * SLOTS, width), BF),
            jax.ShapeDtypeStruct((2, 4 * experts * SLOTS, 2 * rows), BF),
        ),
        in_specs=[pl.BlockSpec(memory_space=pltpu.SMEM)] + [vm] * len(flat),
        out_specs=(vm, vm, vm),
        cost_estimate=pl.CostEstimate(
            flops=16 * rows * 2 * experts * SLOTS * width,
            bytes_accessed=16 * rows * width,
            transcendentals=0,
        ),
        name="select",
    )(me, *flat)


def expert_kernel(*refs, pieces):
    xs, (wg, wu, wd), ys = refs[:pieces], refs[pieces : pieces + 3], refs[pieces + 3 :]
    x = jnp.concatenate([ref[0] for ref in xs], axis=0)
    gate = dot(x, wg[0])
    up = dot(x, wu[0])
    hidden = (gate / (1.0 + jnp.exp(-gate)) * up).astype(BF)
    out = dot(hidden, wd[0]).astype(BF)
    n = xs[0].shape[1]
    for j in range(pieces):
        ys[j][0] = out[j * n : (j + 1) * n]


def run_experts(xs, w_gate, w_up, w_down):
    pieces = len(xs)
    experts, n, width = xs[0].shape
    hidden = w_gate.shape[2]
    blk = pl.BlockSpec((1, n, width), lambda e: (e, 0, 0))
    return pl.pallas_call(
        functools.partial(expert_kernel, pieces=pieces),
        grid=(experts,),
        out_shape=[jax.ShapeDtypeStruct(xs[0].shape, BF)] * pieces,
        in_specs=[blk] * pieces
        + [
            pl.BlockSpec((1, width, hidden), lambda e: (e, 0, 0)),
            pl.BlockSpec((1, width, hidden), lambda e: (e, 0, 0)),
            pl.BlockSpec((1, hidden, width), lambda e: (e, 0, 0)),
        ],
        out_specs=[blk] * pieces,
        cost_estimate=pl.CostEstimate(
            flops=6 * experts * pieces * n * width * hidden,
            bytes_accessed=2 * (3 * w_gate.size + 2 * pieces * xs[0].size),
            transcendentals=experts * pieces * n * hidden,
        ),
        name="experts",
    )(*xs, w_gate, w_up, w_down)


def shared_kernel(a_ref, b_ref, gu0_ref, gu1_ref, d0_ref, d1_ref, gv_ref, out_ref, *, rows):
    x = jnp.concatenate([a_ref[0:rows, :], b_ref[0:rows, :]], axis=0)
    total = None
    for gu_ref, d_ref in ((gu0_ref, d0_ref), (gu1_ref, d1_ref)):
        gate = dot(x, gu_ref[0])
        up = dot(x, gu_ref[1])
        hidden = (gate / (1.0 + jnp.exp(-gate)) * up).astype(BF)
        part = dot(hidden, d_ref[...])
        total = part if total is None else total + part
    level = jnp.sum(x.astype(F32) * gv_ref[...].astype(F32), axis=1, keepdims=True)
    total = total * (1.0 / (1.0 + jnp.exp(-level)))
    out_ref[0] = total[0:rows]
    out_ref[1] = total[rows:]


def run_shared(a, b, gate_up, down, gate_vector, rows):
    width = a.shape[1]
    vm = pl.BlockSpec(memory_space=pltpu.VMEM)
    return pl.pallas_call(
        functools.partial(shared_kernel, rows=rows),
        out_shape=jax.ShapeDtypeStruct((2, rows, width), F32),
        in_specs=[vm] * 7,
        out_specs=vm,
        cost_estimate=pl.CostEstimate(
            flops=24 * rows * down[0].size, bytes_accessed=8 * gate_up[0].size, transcendentals=0
        ),
        name="shared",
    )(a, b, *gate_up, *down, gate_vector.reshape(1, width))


def mix_kernel(*refs, rows, counts, with_shared):
    own_ref, back_ref, cw_ref = refs[:3]
    outs = refs[4:] if with_shared else refs[3:]
    pieces, at = [], 0
    for n in counts:
        pieces.append(outs[at : at + n])
        at += n
    for pair in (1, 0):
        span = slice(2 * SLOTS * pair, 2 * SLOTS * (pair + 1))
        y = jnp.concatenate([own_ref[:, span, :], back_ref[:, span, :]], axis=0)
        y = y.reshape(y.shape[0] * y.shape[1], y.shape[2])
        part = dot(cw_ref[pair], y, (((0,), (0,)), ((), ())))
        for b in range(2):
            block = part[b * rows : (b + 1) * rows]
            if with_shared and pair == 0:
                block = block + refs[3][b]
            start = 0
            for dst in pieces[2 * pair + b]:
                dst[...] = block[start : start + dst.shape[0]].astype(BF)
                start += dst.shape[0]


def mix(own, back, cw, rows, shared=None, split=False):
    width = own.shape[2]
    vm = pl.BlockSpec(memory_space=pltpu.VMEM)
    ins = (own, back, cw) if shared is None else (own, back, cw, shared)
    counts = [1, 1, 1, 2 if split else 1]
    full = jax.ShapeDtypeStruct((rows, width), BF)
    part = jax.ShapeDtypeStruct((rows // 2, width), BF)
    return pl.pallas_call(
        functools.partial(
            mix_kernel, rows=rows, counts=counts, with_shared=shared is not None
        ),
        out_shape=[full] * 3 + ([part] * 2 if split else [full]),
        in_specs=[vm] * len(ins),
        out_specs=[vm] * (5 if split else 4),
        cost_estimate=pl.CostEstimate(
            flops=16 * rows * 2 * own.shape[0] * SLOTS * width,
            bytes_accessed=8 * own.size,
            transcendentals=0,
        ),
        name="mix",
    )(*ins)


class Grid:
    def __init__(self, mesh):
        flat = list(mesh.devices.flat)
        self.at = [tuple(d.coords) + (d.core_on_chip,) for d in flat]
        low = [min(p[i] for p in self.at) for i in range(4)]
        self.at = [tuple(p[i] - low[i] for i in range(4)) for p in self.at]
        self.index = {p: i for i, p in enumerate(self.at)}
        self.size = tuple(max(p[i] for p in self.at) + 1 for i in range(4))

    def partner(self, axis, bits):
        moved = [p[:axis] + (p[axis] ^ bits,) + p[axis + 1 :] for p in self.at]
        return [(i, self.index[q]) for i, q in enumerate(moved)]

    def steps(self, axis, hops):
        pairs = []
        for i, p in enumerate(self.at):
            for a, b in hops:
                if p[axis] == a:
                    pairs.append((i, self.index[p[:axis] + (b,) + p[axis + 1 :]]))
        return pairs


def by_neighbours(
    grid,
    tokens,
    expert_ids,
    combine,
    w_gate,
    w_up,
    w_down,
    shared_gate_up,
    shared_down,
    gate_vector,
):
    rows, width = tokens.shape
    top = expert_ids.shape[1]
    experts = w_gate.shape[0]
    depth = grid.size[2]
    half = rows // 2

    def send(value, axis, bits=1):
        return lax.ppermute(value, AXES, grid.partner(axis, bits))

    def line(value, hops):
        return lax.ppermute(value, AXES, grid.steps(2, hops))

    wide = lambda v: v.astype(F32)
    me = lax.axis_index(AXES).astype(jnp.int32).reshape(1)
    flip = grid.partner(3, 1)[0][1]
    per = -(-top // META)

    def tile(values):
        t = jnp.pad(values.T.astype(BF), ((0, per * META - top), (0, 0)))
        return t.reshape(per, META, rows).transpose(1, 0, 2).reshape(META, per * rows)

    meta = jnp.concatenate([tile(expert_ids), tile(combine)], axis=1)
    meta = jnp.pad(meta, ((0, 0), (0, width - meta.shape[1])))
    own = jnp.concatenate([tokens, meta], axis=0)

    mine, theirs, weights = {}, {}, {}
    near = send(own, 2)
    across = line(own, MIDDLE)
    handed = line(near, MIDDLE)
    cols = [own, near, across + line(across, OUT), handed + line(handed, OUT)]
    gate_up = (shared_gate_up, send(shared_gate_up, 3))
    down = (shared_down, send(shared_down, 3))
    shared = None
    for j in range(depth):
        o = cols[j]
        x, y = send(o, 0), send(o, 1)
        path = corner_path(j, depth)
        if path == "split":
            d = (send(x[:half], 1), send(y[half:], 0))
        elif path == "y":
            d = (send(x, 1),)
        else:
            d = (send(y, 0),)
        mine[j], other, weights[j] = select(me, [(o,), (x,), (y,), d], flip, rows, top, experts)
        theirs[j] = send(other, 3)
        if j == 0:
            shared = run_shared(o, x, gate_up, down, gate_vector, rows)

    xs = [mine[j] for j in range(depth)] + [theirs[j] for j in range(depth)]
    outs = run_experts(xs, w_gate, w_up, w_down)

    sums = {}
    for j in reversed(range(depth)):
        back = send(outs[depth + j], 3)
        path = corner_path(j, depth)
        o, x, y, *d = mix(outs[j], back, weights[j], rows, None if j else shared, path == "split")
        if path == "split":
            d0, d1 = wide(send(d[0], 1)), wide(send(d[1], 0))
            x = jnp.concatenate([wide(x[:half]) + d0, wide(x[half:])], axis=0).astype(BF)
            y = jnp.concatenate([wide(y[:half]), wide(y[half:]) + d1], axis=0).astype(BF)
        elif path == "y":
            x = (wide(x) + wide(send(d[0], 1))).astype(BF)
        else:
            y = (wide(y) + wide(send(d[0], 0))).astype(BF)
        sums[j] = wide(o) + wide(send(x, 0)) + wide(send(y, 1))

    handed = (sums[3] + wide(line(sums[3].astype(BF), IN))).astype(BF)
    across = (sums[2] + wide(line(sums[2].astype(BF), IN))).astype(BF)
    near = (sums[1] + wide(line(handed, MIDDLE))).astype(BF)
    total = sums[0] + wide(line(across, MIDDLE)) + wide(send(near, 2))
    return total.astype(BF)


MIDDLE = ((1, 2), (2, 1))
OUT = ((1, 0), (2, 3))
IN = ((0, 1), (3, 2))


def corner_path(j, depth):
    return "split" if j == depth - 1 else "yx"[j % 2]


def solution(mesh):
    grid = Grid(mesh)
    planar = grid.size == (2, 2, 4, 2)

    def body(*args):
        return by_neighbours(grid, *args) if planar else by_all_to_all(*args)

    return jax.shard_map(
        body,
        mesh=mesh,
        in_specs=(
            P(AXES, None),
            P(AXES, None),
            P(AXES, None),
            P(AXES, None, None),
            P(AXES, None, None),
            P(AXES, None, None),
            P(None, None, "narrow"),
            P("narrow", None),
            P(),
        ),
        out_specs=P(AXES, None),
        check_vma=False,
    )
```

```python
import functools
import jax
import jax.numpy as jnp
from jax import lax
from jax.experimental import pallas as pl
from jax.experimental.pallas import tpu as pltpu
from jax.sharding import PartitionSpec as P


CAP = 7
AXES = ("wide", "narrow")
BF = jnp.bfloat16
F32 = jnp.float32
META = 8
SLOTS = 8


def slot_order(flat_ids, experts_total):
    columns = jnp.arange(experts_total, dtype=jnp.int32)
    onehot = (flat_ids[:, None] == columns[None, :]).astype(jnp.int32)
    before = jnp.cumsum(onehot, axis=0) - onehot
    return jnp.sum(before * onehot, axis=1)


def expert_block(received, w_gate, w_up, w_down):
    gate_part = jnp.einsum("secd,edf->secf", received, w_gate, preferred_element_type=F32)
    up_part = jnp.einsum("secd,edf->secf", received, w_up, preferred_element_type=F32)
    hidden = (jax.nn.silu(gate_part) * up_part).astype(BF)
    return jnp.einsum("secf,efd->secd", hidden, w_down, preferred_element_type=F32).astype(BF)


def by_all_to_all(
    tokens, expert_ids, combine, w_gate, w_up, w_down, shared_gate_up, shared_down, gate_vector
):
    tok_rows, model_width = tokens.shape
    top_count = expert_ids.shape[1]
    devices = lax.axis_size(AXES)
    local_experts = w_gate.shape[0]
    experts_total = local_experts * devices
    flat_ids = expert_ids.reshape(-1)
    positions = slot_order(flat_ids, experts_total)
    slot_index = flat_ids * CAP + positions
    repeated = jnp.repeat(tokens, top_count, axis=0)
    outgoing = jnp.zeros((experts_total * CAP, model_width), BF).at[slot_index].set(repeated)
    outgoing = outgoing.reshape(devices, local_experts, CAP, model_width)
    produced = expert_block(
        lax.all_to_all(outgoing, AXES, split_axis=0, concat_axis=0, tiled=True),
        w_gate,
        w_up,
        w_down,
    )
    returned = lax.all_to_all(produced, AXES, split_axis=0, concat_axis=0, tiled=True)
    returned = returned.reshape(experts_total * CAP, model_width)
    returned_rows = returned[slot_index].reshape(tok_rows, top_count, model_width)
    mix_weights = combine.astype(F32) / 256.0
    routed = jnp.sum(returned_rows.astype(F32) * mix_weights[:, :, None], axis=1)
    shared_scale = jax.nn.sigmoid(jnp.dot(tokens, gate_vector, preferred_element_type=F32))
    gate_up = jnp.einsum(
        "td,gdn->gtn",
        tokens,
        lax.all_gather(shared_gate_up, "narrow", axis=2, tiled=True),
        preferred_element_type=F32,
    )
    shared_hidden = (jax.nn.silu(gate_up[0]) * gate_up[1]).astype(BF)
    shared_out = jnp.dot(
        shared_hidden,
        lax.all_gather(shared_down, "narrow", axis=0, tiled=True),
        preferred_element_type=F32,
    )
    layer_out = routed + shared_scale[:, None] * shared_out
    return layer_out.astype(BF)


def dot(a, b, dims=(((1,), (0,)), ((), ()))):
    return lax.dot_general(a, b, dims, preferred_element_type=F32)


def split_block(refs, rows):
    if len(refs) == 1:
        return refs[0][0:rows, :], refs[0][rows : rows + META, :]
    top, rest = refs
    cut = rows - top.shape[0]
    return jnp.concatenate([top[...], rest[0:cut, :]], axis=0), rest[cut : cut + META, :]


def select_kernel(me_ref, *refs, counts, flip, rows, top, experts):
    blocks, at = [], 0
    for n in counts:
        blocks.append(split_block(refs[at : at + n], rows))
        at += n
    own_ref, sib_ref, cw_ref = refs[at:]
    r = lax.broadcasted_iota(jnp.int32, (rows, rows), 0)
    c = lax.broadcasted_iota(jnp.int32, (rows, rows), 1)
    upper = jnp.where(r < c, 1.0, 0.0).astype(BF)
    e = lax.broadcasted_iota(jnp.int32, (2 * experts, 1, rows), 0)
    me = me_ref[0]
    sib = jnp.bitwise_xor(me, flip)
    mine = jnp.where(e < experts, e + me * experts, e - experts + sib * experts).astype(F32)
    slot = lax.broadcasted_iota(jnp.int32, (2 * experts, SLOTS, rows), 1).astype(F32)
    zero = jnp.zeros((2 * experts, SLOTS, rows), F32)
    per = -(-top // META)

    def table(meta, at):
        parts = []
        for k0 in range(0, top, META):
            n = min(META, top - k0)
            lanes = (at + k0 // META) * rows
            parts.append(meta[0:n, lanes : lanes + rows])
        return jnp.concatenate(parts, axis=0)

    def spread(pieces):
        wide = [jnp.concatenate([pieces[0], zero], 2), jnp.concatenate([zero, pieces[1]], 2)]
        both = jnp.concatenate(wide, axis=1)
        return both.reshape(4 * experts * SLOTS, 2 * rows).astype(BF)

    for pair in range(2):
        halves, weighted = [], []
        for toks, meta in blocks[2 * pair : 2 * pair + 2]:
            meta = meta[:, 0 : 2 * per * rows].astype(F32)
            ids, part = table(meta, 0), table(meta, per)
            match = jnp.where(ids[None] == mine, 1.0, 0.0)
            hit = jnp.sum(match, axis=1)
            part_of = jnp.sum(match * part[None], axis=1) * (1.0 / 256.0)
            before = dot(hit.astype(BF), upper)
            here = jnp.where((before[:, None, :] == slot) & (hit[:, None, :] > 0.0), 1.0, 0.0)
            halves.append(here)
            weighted.append(here * part_of[:, None, :])
        cw_ref[pair] = spread(weighted)
        toks = jnp.concatenate([blocks[2 * pair][0], blocks[2 * pair + 1][0]], axis=0)
        picked = dot(spread(halves), toks).astype(BF)
        picked = picked.reshape(2 * experts, 2 * SLOTS, picked.shape[1])
        own_ref[:, 2 * SLOTS * pair : 2 * SLOTS * (pair + 1), :] = picked[:experts]
        sib_ref[:, 2 * SLOTS * pair : 2 * SLOTS * (pair + 1), :] = picked[experts:]


def select(me, blocks, flip, rows, top, experts):
    width = blocks[0][0].shape[1]
    vm = pl.BlockSpec(memory_space=pltpu.VMEM)
    flat = [piece for block in blocks for piece in block]
    return pl.pallas_call(
        functools.partial(
            select_kernel,
            counts=[len(b) for b in blocks],
            flip=flip,
            rows=rows,
            top=top,
            experts=experts,
        ),
        out_shape=(
            jax.ShapeDtypeStruct((experts, 4 * SLOTS, width), BF),
            jax.ShapeDtypeStruct((experts, 4 * SLOTS, width), BF),
            jax.ShapeDtypeStruct((2, 4 * experts * SLOTS, 2 * rows), BF),
        ),
        in_specs=[pl.BlockSpec(memory_space=pltpu.SMEM)] + [vm] * len(flat),
        out_specs=(vm, vm, vm),
        cost_estimate=pl.CostEstimate(
            flops=16 * rows * 2 * experts * SLOTS * width,
            bytes_accessed=16 * rows * width,
            transcendentals=0,
        ),
        name="select",
    )(me, *flat)


def expert_kernel(*refs, pieces):
    xs, (wg, wu, wd), ys = refs[:pieces], refs[pieces : pieces + 3], refs[pieces + 3 :]
    x = jnp.concatenate([ref[0] for ref in xs], axis=0)
    gate = dot(x, wg[0])
    up = dot(x, wu[0])
    hidden = (gate / (1.0 + jnp.exp(-gate)) * up).astype(BF)
    out = dot(hidden, wd[0]).astype(BF)
    n = xs[0].shape[1]
    for j in range(pieces):
        ys[j][0] = out[j * n : (j + 1) * n]


def run_experts(xs, w_gate, w_up, w_down):
    pieces = len(xs)
    experts, n, width = xs[0].shape
    hidden = w_gate.shape[2]
    blk = pl.BlockSpec((1, n, width), lambda e: (e, 0, 0))
    return pl.pallas_call(
        functools.partial(expert_kernel, pieces=pieces),
        grid=(experts,),
        out_shape=[jax.ShapeDtypeStruct(xs[0].shape, BF)] * pieces,
        in_specs=[blk] * pieces
        + [
            pl.BlockSpec((1, width, hidden), lambda e: (e, 0, 0)),
            pl.BlockSpec((1, width, hidden), lambda e: (e, 0, 0)),
            pl.BlockSpec((1, hidden, width), lambda e: (e, 0, 0)),
        ],
        out_specs=[blk] * pieces,
        cost_estimate=pl.CostEstimate(
            flops=6 * experts * pieces * n * width * hidden,
            bytes_accessed=2 * (3 * w_gate.size + 2 * pieces * xs[0].size),
            transcendentals=experts * pieces * n * hidden,
        ),
        name="experts",
    )(*xs, w_gate, w_up, w_down)


def shared_kernel(a_ref, b_ref, gu0_ref, gu1_ref, d0_ref, d1_ref, gv_ref, out_ref, *, rows):
    x = jnp.concatenate([a_ref[0:rows, :], b_ref[0:rows, :]], axis=0)
    total = None
    for gu_ref, d_ref in ((gu0_ref, d0_ref), (gu1_ref, d1_ref)):
        gate = dot(x, gu_ref[0])
        up = dot(x, gu_ref[1])
        hidden = (gate / (1.0 + jnp.exp(-gate)) * up).astype(BF)
        part = dot(hidden, d_ref[...])
        total = part if total is None else total + part
    level = jnp.sum(x.astype(F32) * gv_ref[...].astype(F32), axis=1, keepdims=True)
    total = total * (1.0 / (1.0 + jnp.exp(-level)))
    out_ref[0] = total[0:rows]
    out_ref[1] = total[rows:]


def run_shared(a, b, gate_up, down, gate_vector, rows):
    width = a.shape[1]
    vm = pl.BlockSpec(memory_space=pltpu.VMEM)
    return pl.pallas_call(
        functools.partial(shared_kernel, rows=rows),
        out_shape=jax.ShapeDtypeStruct((2, rows, width), F32),
        in_specs=[vm] * 7,
        out_specs=vm,
        cost_estimate=pl.CostEstimate(
            flops=24 * rows * down[0].size, bytes_accessed=8 * gate_up[0].size, transcendentals=0
        ),
        name="shared",
    )(a, b, *gate_up, *down, gate_vector.reshape(1, width))


def mix_kernel(*refs, rows, counts, with_shared):
    own_ref, back_ref, cw_ref = refs[:3]
    outs = refs[4:] if with_shared else refs[3:]
    pieces, at = [], 0
    for n in counts:
        pieces.append(outs[at : at + n])
        at += n
    for pair in (1, 0):
        span = slice(2 * SLOTS * pair, 2 * SLOTS * (pair + 1))
        y = jnp.concatenate([own_ref[:, span, :], back_ref[:, span, :]], axis=0)
        y = y.reshape(y.shape[0] * y.shape[1], y.shape[2])
        part = dot(cw_ref[pair], y, (((0,), (0,)), ((), ())))
        for b in range(2):
            block = part[b * rows : (b + 1) * rows]
            if with_shared and pair == 0:
                block = block + refs[3][b]
            start = 0
            for dst in pieces[2 * pair + b]:
                dst[...] = block[start : start + dst.shape[0]].astype(BF)
                start += dst.shape[0]


def mix(own, back, cw, rows, shared=None, split=False):
    width = own.shape[2]
    vm = pl.BlockSpec(memory_space=pltpu.VMEM)
    ins = (own, back, cw) if shared is None else (own, back, cw, shared)
    counts = [1, 1, 1, 2 if split else 1]
    full = jax.ShapeDtypeStruct((rows, width), BF)
    part = jax.ShapeDtypeStruct((rows // 2, width), BF)
    return pl.pallas_call(
        functools.partial(
            mix_kernel, rows=rows, counts=counts, with_shared=shared is not None
        ),
        out_shape=[full] * 3 + ([part] * 2 if split else [full]),
        in_specs=[vm] * len(ins),
        out_specs=[vm] * (5 if split else 4),
        cost_estimate=pl.CostEstimate(
            flops=16 * rows * 2 * own.shape[0] * SLOTS * width,
            bytes_accessed=8 * own.size,
            transcendentals=0,
        ),
        name="mix",
    )(*ins)


class Grid:
    def __init__(self, mesh):
        flat = list(mesh.devices.flat)
        self.at = [tuple(d.coords) + (d.core_on_chip,) for d in flat]
        low = [min(p[i] for p in self.at) for i in range(4)]
        self.at = [tuple(p[i] - low[i] for i in range(4)) for p in self.at]
        self.index = {p: i for i, p in enumerate(self.at)}
        self.size = tuple(max(p[i] for p in self.at) + 1 for i in range(4))

    def partner(self, axis, bits):
        moved = [p[:axis] + (p[axis] ^ bits,) + p[axis + 1 :] for p in self.at]
        return [(i, self.index[q]) for i, q in enumerate(moved)]

    def steps(self, axis, hops):
        pairs = []
        for i, p in enumerate(self.at):
            for a, b in hops:
                if p[axis] == a:
                    pairs.append((i, self.index[p[:axis] + (b,) + p[axis + 1 :]]))
        return pairs


def by_neighbours(
    grid,
    tokens,
    expert_ids,
    combine,
    w_gate,
    w_up,
    w_down,
    shared_gate_up,
    shared_down,
    gate_vector,
):
    rows, width = tokens.shape
    top = expert_ids.shape[1]
    experts = w_gate.shape[0]
    depth = grid.size[2]
    half = rows // 2

    def send(value, axis, bits=1):
        return lax.ppermute(value, AXES, grid.partner(axis, bits))

    def line(value, hops):
        return lax.ppermute(value, AXES, grid.steps(2, hops))

    wide = lambda v: v.astype(F32)
    me = lax.axis_index(AXES).astype(jnp.int32).reshape(1)
    flip = grid.partner(3, 1)[0][1]
    per = -(-top // META)

    def tile(values):
        t = jnp.pad(values.T.astype(BF), ((0, per * META - top), (0, 0)))
        return t.reshape(per, META, rows).transpose(1, 0, 2).reshape(META, per * rows)

    meta = jnp.concatenate([tile(expert_ids), tile(combine)], axis=1)
    meta = jnp.pad(meta, ((0, 0), (0, width - meta.shape[1])))
    own = jnp.concatenate([tokens, meta], axis=0)

    mine, theirs, weights = {}, {}, {}
    near = send(own, 2)
    across = line(own, MIDDLE)
    handed = line(near, MIDDLE)
    cols = [own, near, across + line(across, OUT), handed + line(handed, OUT)]
    gate_up = (shared_gate_up, send(shared_gate_up, 3))
    down = (shared_down, send(shared_down, 3))
    shared = None
    for j in range(depth):
        o = cols[j]
        x, y = send(o, 0), send(o, 1)
        path = corner_path(j, depth)
        if path == "split":
            d = (send(x[:half], 1), send(y[half:], 0))
        elif path == "y":
            d = (send(x, 1),)
        else:
            d = (send(y, 0),)
        mine[j], other, weights[j] = select(me, [(o,), (x,), (y,), d], flip, rows, top, experts)
        theirs[j] = send(other, 3)
        if j == 0:
            shared = run_shared(o, x, gate_up, down, gate_vector, rows)

    xs = [mine[j] for j in range(depth)] + [theirs[j] for j in range(depth)]
    outs = run_experts(xs, w_gate, w_up, w_down)

    sums = {}
    for j in reversed(range(depth)):
        back = send(outs[depth + j], 3)
        path = corner_path(j, depth)
        o, x, y, *d = mix(outs[j], back, weights[j], rows, None if j else shared, path == "split")
        if path == "split":
            d0, d1 = wide(send(d[0], 1)), wide(send(d[1], 0))
            x = (wide(x) + jnp.pad(d0, ((0, rows - half), (0, 0)))).astype(BF)
            y = (wide(y) + jnp.pad(d1, ((half, 0), (0, 0)))).astype(BF)
        elif path == "y":
            x = (wide(x) + wide(send(d[0], 1))).astype(BF)
        else:
            y = (wide(y) + wide(send(d[0], 0))).astype(BF)
        sums[j] = wide(o) + wide(send(x, 0)) + wide(send(y, 1))

    handed = (sums[3] + wide(line(sums[3].astype(BF), IN))).astype(BF)
    across = (sums[2] + wide(line(sums[2].astype(BF), IN))).astype(BF)
    near = (sums[1] + wide(line(handed, MIDDLE))).astype(BF)
    total = sums[0] + wide(line(across, MIDDLE)) + wide(send(near, 2))
    return total.astype(BF)


MIDDLE = ((1, 2), (2, 1))
OUT = ((1, 0), (2, 3))
IN = ((0, 1), (3, 2))


def corner_path(j, depth):
    return "split" if j >= depth // 2 else "yx"[j % 2]


def solution(mesh):
    grid = Grid(mesh)
    planar = grid.size == (2, 2, 4, 2)

    def body(*args):
        return by_neighbours(grid, *args) if planar else by_all_to_all(*args)

    return jax.shard_map(
        body,
        mesh=mesh,
        in_specs=(
            P(AXES, None),
            P(AXES, None),
            P(AXES, None),
            P(AXES, None, None),
            P(AXES, None, None),
            P(AXES, None, None),
            P(None, None, "narrow"),
            P("narrow", None),
            P(),
        ),
        out_specs=P(AXES, None),
        check_vma=False,
    )
```
